32 devices in a mesh: row: 8 (over z, core), col: 4 (over y, x).
Axes of the slice: x: 2, y: 2, z: 4, core: 2. Of those that a mesh axis runs over, the one named last changes fastest.
Arguments:
- u_start: float32 [128, 131072], P('col', 'row'), may hold values from -24 to 24
- v_start: float32 [128, 65536], P('row', 'col'), may hold values from -24 to 24
- keep_u: float32 [128, 40], replicated, may hold values from -1 to 1, as said below
- keep_v: float32 [128, 40], replicated, may hold values from -1 to 1, as said below
- v_next: float32 [65536], P(('col', 'row')), may hold values from -96 to 96
- tile_blocks: bfloat16 [2048, 256, 256], P(('row', 'col')), may hold values from -0.375 to 0.375
- tile_rows: int32 [2048], P(('row', 'col')), may hold values from 0 to 63
- tile_cols: int32 [2048], P(('row', 'col')), may hold values from 0 to 63
- tile_count: int32 [32], P(('row', 'col')), may hold values from 32 to 64
Outputs:
- u_basis: float32 [42, 131072], P(None, ('row', 'col'))
- v_basis: float32 [43, 65536], P(None, ('col', 'row'))
- bidiagonal: float32 [2, 2], replicated
The draws below stay inside these ranges and needn't reach their ends.
Inputs may be any that keep to these rules, and one draw needn't show every extreme that they name: `tile_rows`: tile row within the device's row group. `tile_cols`: tile column within the device's column group. `tile_count`: slots at this index and beyond hold no tile. `keep_u`: the columns are orthonormal. `keep_v`: the columns are orthonormal.
All inputs are finite; a program needn't handle non-finite values.
Results may differ from the reference program's by a relative error of at most 0.00155.
Values may be sent and summed in bfloat16 or wider, within the bound.
A program may use at most 64 MiB of HBM per device.

```python
import jax
import jax.numpy as jnp
from jax import lax

BASIS = 128
KEEP = 40
TILE = 256
STEPS = 2
RB = 64
CB = 64
TILES_DEV = 64
M = 131072
N = 65536
TILES = 2048
N_COL = 4
DEVICES = 32


def basis_rows_draw(key, count, length):
    raw = jax.random.normal(jax.random.fold_in(key, 1), (length, count), jnp.float32)
    factor, upper = jnp.linalg.qr(raw)
    rows = factor.T * jnp.sqrt(jnp.float32(length))
    along = jnp.arange(length, dtype=jnp.float32) / jnp.float32(length)
    inner = along * jnp.float32(N_COL) - jnp.floor(along * jnp.float32(N_COL))
    weight = (1.0 + 2.0 * along) * (1.0 + 2.0 * inner)
    row_scale = jax.random.uniform(jax.random.fold_in(key, 2), (count, 1), jnp.float32, 0.7, 1.3)
    rows = rows * weight[None, :]
    rows = rows / jnp.sqrt(jnp.mean(rows * rows, axis=1, keepdims=True))
    rows = rows * row_scale
    return jnp.clip(rows, -24.0, 24.0).astype(jnp.float32)


def columns_draw(key, count, width):
    raw = jax.random.normal(key, (count, width), jnp.float32)
    factor, upper = jnp.linalg.qr(raw)
    return factor.astype(jnp.float32)


def draw_u_start(key, part):
    return basis_rows_draw(jax.random.fold_in(key, 11), BASIS, M)


def draw_v_start(key, part):
    return basis_rows_draw(jax.random.fold_in(key, 23), BASIS, N)


def draw_keep_u(key, part):
    return columns_draw(jax.random.fold_in(key, 37), BASIS, KEEP)


def draw_keep_v(key, part):
    return columns_draw(jax.random.fold_in(key, 41), BASIS, KEEP)


def draw_v_next(key, part):
    rows = basis_rows_draw(jax.random.fold_in(key, 23), BASIS, N)
    mixing = 0.5 * jax.random.normal(jax.random.fold_in(key, 59), (BASIS,), jnp.float32)
    noise = jax.random.normal(jax.random.fold_in(key, 61), (N,), jnp.float32)
    mixed = noise + jnp.dot(mixing, rows, precision=jax.lax.Precision.HIGHEST)
    return jnp.clip(mixed, -96.0, 96.0).astype(jnp.float32)


def plant(entries, stream_key, low, high):
    spot = [jax.random.randint(jax.random.fold_in(stream_key, axis), (), 0, length) for axis, length in enumerate(entries.shape)]
    longest = entries.shape.index(max(entries.shape))
    neighbour = spot[:longest] + [(spot[longest] + 1) % entries.shape[longest]] + spot[longest + 1:]
    return entries.at[tuple(spot)].set(low).at[tuple(neighbour)].set(high)


def level_of(own_key, extent, pieces, low, largest):
    def one(position, blocks):
        heights = jax.random.uniform(jax.random.fold_in(jax.random.fold_in(own_key, 6), position), (blocks,), jnp.float32, low / len(pieces), largest / len(pieces))
        return jnp.repeat(jnp.exp(heights), extent[position] // blocks).reshape((-1,) + (1,) * (len(extent) - position - 1))

    level = one(*pieces[0])
    for cut in pieces[1:]:
        level = level * one(*cut)
    return level


def scatter_about(rng, shape, deviation, limit, shards=(), kind=jnp.bfloat16):
    gain = level_of(rng, shape, shards, -0.22, 0.18) if shards else 1.0
    array = jax.random.normal(rng, shape, jnp.float32) * deviation * gain
    return jnp.minimum(jnp.maximum(array, -limit), limit).astype(kind)


def setup_inputs(seed: int = 0) -> dict:
    splits = jax.random.split(jax.random.key(seed), 10)
    u_start = draw_u_start(jax.random.fold_in(splits[9], 71), 0)
    v_start = draw_v_start(jax.random.fold_in(splits[9], 71), 0)
    keep_u = draw_keep_u(jax.random.fold_in(splits[9], 71), 0)
    keep_v = draw_keep_v(jax.random.fold_in(splits[9], 71), 0)
    v_next = draw_v_next(jax.random.fold_in(splits[9], 71), 0)
    tile_blocks = scatter_about(splits[5], (TILES, TILE, TILE), TILE ** -0.5, 0.375, ((0, 32),))
    tile_rows = plant(jax.random.randint(splits[6], (TILES,), 0, RB), jax.random.fold_in(splits[6], 1), 0, RB - 1).astype(jnp.int32)
    tile_cols = plant(jax.random.randint(splits[7], (TILES,), 0, CB), jax.random.fold_in(splits[7], 1), 0, CB - 1).astype(jnp.int32)
    tile_count = plant(jax.random.randint(splits[8], (DEVICES,), TILES_DEV // 2, TILES_DEV + 1), jax.random.fold_in(splits[8], 1), TILES_DEV // 2, TILES_DEV).astype(jnp.int32)
    return {"u_start": u_start, "v_start": v_start, "keep_u": keep_u, "keep_v": keep_v, "v_next": v_next, "tile_blocks": tile_blocks, "tile_rows": tile_rows, "tile_cols": tile_cols, "tile_count": tile_count}


HIGH = lax.Precision.HIGHEST

def tile_product(tile_blocks, tile_rows, tile_cols, tile_count, vector, forward_pass):
    rounded = lax.optimization_barrier(vector.astype(jnp.bfloat16)).astype(jnp.float32)
    if forward_pass:
        blocks = rounded.reshape(N // TILE, TILE)
        segments = M // TILE
    else:
        blocks = rounded.reshape(M // TILE, TILE)
        segments = N // TILE
    grouped = tile_blocks.reshape(DEVICES, TILES_DEV, TILE, TILE)
    row_slots = tile_rows.reshape(DEVICES, TILES_DEV)
    col_slots = tile_cols.reshape(DEVICES, TILES_DEV)

    def per_device(device):
        row_group = device // N_COL
        col_group = device % N_COL
        tile_float = lax.dynamic_index_in_dim(grouped, device, 0, keepdims=False).astype(jnp.float32)
        local_rows = lax.dynamic_index_in_dim(row_slots, device, 0, keepdims=False)
        local_cols = lax.dynamic_index_in_dim(col_slots, device, 0, keepdims=False)
        active = (jnp.arange(TILES_DEV, dtype=jnp.int32) < tile_count[device]).astype(jnp.float32)
        row_index = (row_group * RB + local_rows).astype(jnp.int32)
        col_index = (col_group * CB + local_cols).astype(jnp.int32)
        if forward_pass:
            picked = blocks[col_index]
            outputs = jnp.einsum('tij,tj->ti', tile_float, picked, precision=HIGH)
            target = row_index
        else:
            picked = blocks[row_index]
            outputs = jnp.einsum('tij,ti->tj', tile_float, picked, precision=HIGH)
            target = col_index
        return (outputs * active[:, None], target)
    outputs, target = lax.map(per_device, jnp.arange(DEVICES, dtype=jnp.int32))
    summed = jax.ops.segment_sum(outputs.reshape(-1, TILE), target.reshape(-1), num_segments=segments)
    return summed.reshape(-1)

def orthonormal(basis_rows, vector):
    length = vector.shape[0]
    first_coef = jnp.dot(basis_rows, vector, precision=HIGH) / length
    once_clean = vector - jnp.dot(first_coef, basis_rows, precision=HIGH)
    second_coef = jnp.dot(basis_rows, once_clean, precision=HIGH) / length
    twice_clean = once_clean - jnp.dot(second_coef, basis_rows, precision=HIGH)
    scale_now = jnp.sqrt(jnp.sum(twice_clean * twice_clean) / length + 1e-06)
    return (twice_clean / scale_now, scale_now)

def reference(u_start, v_start, keep_u, keep_v, v_next, tile_blocks, tile_rows, tile_cols, tile_count):
    u_kept = jnp.dot(keep_u.T, u_start, precision=HIGH)
    v_kept = jnp.dot(keep_v.T, v_start, precision=HIGH)
    first_right, beta_start = orthonormal(v_kept, v_next)
    left_rows = u_kept
    right_rows = jnp.concatenate([v_kept, first_right[None, :]], axis=0)
    current = first_right
    alpha_list = []
    beta_list = []
    for iteration in range(STEPS):
        image = tile_product(tile_blocks, tile_rows, tile_cols, tile_count, current, True)
        left_new, alpha = orthonormal(left_rows, image)
        left_rows = jnp.concatenate([left_rows, left_new[None, :]], axis=0)
        back_image = tile_product(tile_blocks, tile_rows, tile_cols, tile_count, left_new, False)
        current, beta = orthonormal(right_rows, back_image)
        right_rows = jnp.concatenate([right_rows, current[None, :]], axis=0)
        alpha_list.append(alpha)
        beta_list.append(beta)
    bidiagonal = jnp.stack([jnp.stack(alpha_list), jnp.stack(beta_list)])
    return (left_rows, right_rows, bidiagonal)
```

```python
import functools

import jax
import jax.numpy as jnp
from jax import lax
from jax.experimental import pallas as pl
from jax.experimental.pallas import tpu as pltpu
from jax.sharding import PartitionSpec as P

STEPS = 2
HIGH = lax.Precision.HIGHEST
F32 = jnp.float32
BF16 = jnp.bfloat16
LANE = 128
HALF = 64


def kernel(
    row_n, col_n, keep_n, u_hbm, v_hbm, keep_u, keep_v, v_next, tiles_hbm, rows_ref, cols_ref, count_ref,
    u_out, v_out, bi_out,
    u_all, v_all, tiles, u_rows, v_rows, u_vec, v_vec, big_col, big_row, sum_col, sum_row,
    v_gather, u_gather, u_parts, v_parts, u_recv, v_recv, picked, products,
    local_sem, init_u_send, init_u_recv, init_v_send, init_v_recv, send_sem,
    sum_col_sem, sum_row_sem, vg_sem, ug_sem, ur_sem, vr_sem,
):
    row_me = lax.axis_index("row")
    col_me = lax.axis_index("col")
    barrier = pltpu.get_barrier_semaphore()
    for k in range(1, row_n):
        pl.semaphore_signal(barrier, inc=1, device_id={"row": lax.rem(row_me + k, row_n)},
                            device_id_type=pl.DeviceIdType.MESH)
    for k in range(1, col_n):
        pl.semaphore_signal(barrier, inc=1, device_id={"col": lax.rem(col_me + k, col_n)},
                            device_id_type=pl.DeviceIdType.MESH)

    u_here, v_here = u_hbm.shape[0], v_hbm.shape[0]
    u_len, v_len = u_rows.shape[1], v_rows.shape[1]
    u_total = float(u_len * row_n * col_n)
    v_total = float(v_len * row_n * col_n)
    rows_p = u_rows.shape[0]
    keep_p = keep_u.shape[0]
    tile = tiles.shape[1]
    slots = tiles.shape[0]
    u_sub, v_sub = u_len // tile, v_len // tile

    def u_src(p):
        return u_hbm.at[:, pl.ds(pl.multiple_of(p * u_len, LANE), u_len)]

    def v_src(p):
        return v_hbm.at[:, pl.ds(pl.multiple_of(p * v_len, LANE), v_len)]

    u_dst = u_all.at[pl.ds(pl.multiple_of(col_me * u_here, 8), u_here), :]
    v_dst = v_all.at[pl.ds(pl.multiple_of(row_me * v_here, 8), v_here), :]
    own_v = pltpu.make_async_copy(v_src(row_me), v_dst, local_sem.at[0])
    own_u = pltpu.make_async_copy(u_src(col_me), u_dst, local_sem.at[1])
    own_t = pltpu.make_async_copy(tiles_hbm, tiles, local_sem.at[2])
    own_v.start()
    own_u.start()
    own_t.start()

    def send(axis, me, n, src, dst, sends, recvs):
        copies = []
        for k in range(1, n):
            target = lax.rem(me + k, n)
            copy = pltpu.make_async_remote_copy(
                src_ref=src(target, k), dst_ref=dst(k), send_sem=sends.at[k], recv_sem=recvs(k),
                device_id={axis: target}, device_id_type=pl.DeviceIdType.MESH)
            copy.start()
            copies.append(copy)
        return copies

    pl.semaphore_wait(barrier, row_n + col_n - 2)
    v_init = send("row", row_me, row_n, lambda p, k: v_src(p), lambda k: v_dst, init_v_send,
                  lambda k: init_v_recv.at[k])
    u_init = send("col", col_me, col_n, lambda p, k: u_src(p), lambda k: u_dst, init_u_send,
                  lambda k: init_u_recv.at[k])

    active = lax.broadcasted_iota(jnp.int32, (1, slots), 1) < count_ref[...]
    row_blocks = u_parts.shape[0] * u_sub
    col_blocks = v_parts.shape[0] * v_sub
    row_hot = jnp.where(
        (lax.broadcasted_iota(jnp.int32, (row_blocks, slots), 0) == rows_ref[...]) & active, 1.0, 0.0)
    col_hot = jnp.where(
        (lax.broadcasted_iota(jnp.int32, (col_blocks, slots), 0) == cols_ref[...]) & active, 1.0, 0.0)

    eye = (lax.broadcasted_iota(jnp.int32, (rows_p, LANE), 0)
           == lax.broadcasted_iota(jnp.int32, (rows_p, LANE), 1))
    row_id = lax.broadcasted_iota(jnp.int32, (rows_p, LANE), 0)
    lane_id = lax.broadcasted_iota(jnp.int32, (rows_p, LANE), 1)
    lane_row = lax.broadcasted_iota(jnp.int32, (1, LANE), 1)

    def to_row(column):
        return jnp.sum(jnp.where(eye, column, 0.0), axis=0, keepdims=True)

    def to_column(row):
        return jnp.sum(jnp.where(eye, row, 0.0), axis=1, keepdims=True)

    def all_sum(value, index, col_buf, row_buf):
        col_buf[col_me] = value
        for copy in send("col", col_me, col_n, lambda p, k: col_buf.at[col_me],
                         lambda k: col_buf.at[col_me], send_sem, lambda k: sum_col_sem.at[index, k]):
            copy.wait()
        total = col_buf[0]
        for i in range(1, col_n):
            total = total + col_buf[i]
        row_buf[row_me] = total
        for copy in send("row", row_me, row_n, lambda p, k: row_buf.at[row_me],
                         lambda k: row_buf.at[row_me], send_sem, lambda k: sum_row_sem.at[index, k]):
            copy.wait()
        total = row_buf[0]
        for i in range(1, row_n):
            total = total + row_buf[i]
        return total

    def small_sum(row, index):
        value = jnp.broadcast_to(row, (8, LANE))
        return all_sum(value, index, sum_col.at[index - 1], sum_row.at[index - 1])[0:1, :]

    def coef(basis, vec):
        acc = jnp.zeros((rows_p, LANE), F32)
        for j in range(vec.shape[1] // LANE):
            at = slice(j * LANE, (j + 1) * LANE)
            acc = acc + basis[:, at] * vec[:, at]
        return to_row(jnp.sum(acc, axis=1, keepdims=True))

    def remove(basis, vec, column):
        spread = jnp.broadcast_to(column, (rows_p, LANE))
        square = jnp.zeros((1, LANE), F32)
        for j in range(vec.shape[1] // LANE):
            at = slice(j * LANE, (j + 1) * LANE)
            new = vec[:, at] - jnp.sum(spread * basis[:, at], axis=0, keepdims=True)
            vec[:, at] = new
            square = square + new * new
        return jnp.sum(square, axis=1, keepdims=True)

    def orth(basis, vec, first_sum, index, length, gram, place):
        first = first_sum / length
        square = remove(basis, vec, to_column(first))
        sent = coef(basis, vec) + jnp.where(lane_row == LANE - 1, square, 0.0)
        got = small_sum(sent, index)
        square = jnp.sum(jnp.where(lane_row == LANE - 1, got, 0.0), axis=1, keepdims=True) / length
        second = jnp.where(lane_row < rows_p, got, 0.0) / length
        second_col = to_column(second)
        gram_coef = jnp.sum(gram * second_col, axis=0, keepdims=True)
        square = (square - 2.0 * jnp.sum(second * second, axis=1, keepdims=True)
                  + jnp.sum(second * gram_coef, axis=1, keepdims=True))
        remove(basis, vec, second_col)
        scale = jnp.sqrt(square + 1e-06)
        inverse = 1.0 / scale
        cross = (second - gram_coef) * inverse
        gram = jnp.where(row_id == place, cross, gram)
        gram = jnp.where(lane_id == place, to_column(cross), gram)
        gram = jnp.where((row_id == place) & (lane_id == place), square / (scale * scale), gram)
        new = vec[...] * inverse
        basis[place:place + 1, :] = new
        vec[...] = new
        return scale, gram

    def matvec(gathered, n, pick_hot, put_hot, contract):
        full = jnp.concatenate([gathered[i].astype(F32) for i in range(n)], axis=0).astype(BF16)
        picked[...] = lax.dot_general(pick_hot.astype(BF16), full, (((0,), (0,)), ((), ())),
                                      preferred_element_type=F32)
        sub = lax.broadcasted_iota(jnp.int32, (8, tile), 0)

        def group(g, carry):
            base = pl.multiple_of(g * 8, 8)
            left = picked[pl.ds(base, 8), :].astype(BF16)
            acc = jnp.zeros((8, tile), F32)
            for i in range(8):
                res = lax.dot_general(left, tiles[base + i], (((1,), (contract,)), ((), ())),
                                      preferred_element_type=F32)
                acc = jnp.where(sub == i, res, acc)
            products[pl.ds(base, 8), :] = acc
            return carry

        lax.fori_loop(0, slots // 8, group, 0)
        return jnp.dot(put_hot, products[...], precision=HIGH, preferred_element_type=F32)

    def gather(axis, me, n, vec, sub, buf, sems):
        own = jnp.concatenate([vec[:, i * tile:(i + 1) * tile] for i in range(sub)], axis=0)
        buf[me] = own.astype(BF16)
        for copy in send(axis, me, n, lambda p, k: buf.at[me], lambda k: buf.at[me], send_sem, sems):
            copy.wait()

    def scatter(axis, me, n, value, vec, sub, parts, recv, sems):
        for i in range(n):
            parts[i] = value[i * sub:(i + 1) * sub, :]
        for copy in send(axis, me, n, lambda p, k: parts.at[p], lambda k: recv.at[k], send_sem, sems):
            copy.wait()
        total = parts[me]
        for k in range(1, n):
            total = total + recv[k]
        for i in range(sub):
            vec[:, i * tile:(i + 1) * tile] = total[i:i + 1, :]

    u_rows[...] = jnp.zeros(u_rows.shape, F32)
    v_rows[...] = jnp.zeros(v_rows.shape, F32)
    v_vec[...] = v_next[...]
    own_v.wait()
    for copy in v_init:
        copy.wait()

    def kept(keep, source, target, length):
        for j in range(length // 512):
            at = slice(j * 512, (j + 1) * 512)
            target[0:keep_p, at] = jnp.dot(keep[...], source[:, at], precision=HIGH,
                                           preferred_element_type=F32)

    def half_gram(basis):
        small = basis[0:keep_p, :]
        wide = jnp.concatenate([basis[...], jnp.zeros((HALF - rows_p, basis.shape[1]), F32)], axis=0)
        return lax.dot_general(small, wide, (((1,), (1,)), ((), ())), precision=HIGH,
                               preferred_element_type=F32)

    kept(keep_v, v_all, v_rows, v_len)
    gram_v = half_gram(v_rows)
    first = coef(v_rows, v_vec)
    own_u.wait()
    for copy in u_init:
        copy.wait()
    kept(keep_u, u_all, u_rows, u_len)
    gram_u = half_gram(u_rows)
    payload = jnp.concatenate(
        [jnp.concatenate([gram_v, gram_u], axis=1), jnp.broadcast_to(first, (8, LANE))], axis=0)
    summed = all_sum(payload, 0, big_col, big_row)
    both = jnp.concatenate([summed[0:keep_p, :], jnp.zeros((rows_p - keep_p, LANE), F32)], axis=0)
    gram_v = jnp.where(lane_id < HALF, both, 0.0) / v_total
    gram_u = jnp.where(lane_id < HALF, pltpu.roll(both, HALF, 1), 0.0) / u_total

    scale, gram_v = orth(v_rows, v_vec, summed[keep_p:keep_p + 1, :], 1, v_total, gram_v, keep_n)
    own_t.wait()
    index = 2
    alphas, betas = [], []
    for step in range(STEPS):
        gather("row", row_me, row_n, v_vec, v_sub, v_gather.at[step], lambda k: vg_sem.at[step, k])
        partial = matvec(v_gather.at[step], row_n, col_hot, row_hot, 1)
        scatter("col", col_me, col_n, partial, u_vec, u_sub, u_parts, u_recv.at[step],
                lambda k: ur_sem.at[step, k])
        alpha, gram_u = orth(u_rows, u_vec, small_sum(coef(u_rows, u_vec), index), index + 1, u_total,
                             gram_u, keep_n + step)
        gather("col", col_me, col_n, u_vec, u_sub, u_gather.at[step], lambda k: ug_sem.at[step, k])
        partial = matvec(u_gather.at[step], col_n, row_hot, col_hot, 0)
        scatter("row", row_me, row_n, partial, v_vec, v_sub, v_parts, v_recv.at[step],
                lambda k: vr_sem.at[step, k])
        beta, gram_v = orth(v_rows, v_vec, small_sum(coef(v_rows, v_vec), index + 2), index + 3,
                            v_total, gram_v, keep_n + 1 + step)
        index += 4
        alphas.append(alpha)
        betas.append(beta)
    place_r = lax.broadcasted_iota(jnp.int32, (8, LANE), 0)
    place_l = lax.broadcasted_iota(jnp.int32, (8, LANE), 1)
    result = jnp.zeros((8, LANE), F32)
    for step in range(STEPS):
        result = jnp.where((place_r == 0) & (place_l == step), alphas[step], result)
        result = jnp.where((place_r == 1) & (place_l == step), betas[step], result)
    bi_out[...] = result
    u_out[...] = u_rows[0:u_out.shape[0], :]
    v_out[...] = v_rows[0:v_out.shape[0], :]


def per_device(
    u_start, v_start, keep_u, keep_v, v_next, tile_blocks, tile_rows, tile_cols, tile_count
):
    row_n = lax.axis_size("row")
    col_n = lax.axis_size("col")
    u_here, v_here = u_start.shape[0], v_start.shape[0]
    basis, keep_n = keep_u.shape
    u_len = u_start.shape[1] // col_n
    v_len = v_start.shape[1] // row_n
    slots, tile = tile_blocks.shape[0], tile_blocks.shape[1]
    rows_p = -(-(keep_n + 1 + STEPS) // 8) * 8
    keep_p = -(-keep_n // 8) * 8
    assert rows_p <= HALF
    pad = ((0, keep_p - keep_n), (0, 0))
    sums = 1 + 4 * STEPS
    dma = pltpu.SemaphoreType.DMA
    vmem = pl.BlockSpec(memory_space=pltpu.VMEM)
    hbm = pl.BlockSpec(memory_space=pl.ANY)
    u_sub, v_sub = u_len // tile, v_len // tile
    u_basis, v_basis, bidiagonal = pl.pallas_call(
        functools.partial(kernel, row_n, col_n, keep_n),
        out_shape=(
            jax.ShapeDtypeStruct((keep_n + STEPS, u_len), F32),
            jax.ShapeDtypeStruct((keep_n + 1 + STEPS, v_len), F32),
            jax.ShapeDtypeStruct((8, LANE), F32),
        ),
        in_specs=[hbm, hbm, vmem, vmem, vmem, hbm, vmem, vmem, vmem],
        out_specs=(vmem, vmem, vmem),
        scratch_shapes=[
            pltpu.VMEM((basis, u_len), F32),
            pltpu.VMEM((basis, v_len), F32),
            pltpu.VMEM(tile_blocks.shape, BF16),
            pltpu.VMEM((rows_p, u_len), F32),
            pltpu.VMEM((rows_p, v_len), F32),
            pltpu.VMEM((1, u_len), F32),
            pltpu.VMEM((1, v_len), F32),
            pltpu.VMEM((col_n, keep_p + 8, LANE), F32),
            pltpu.VMEM((row_n, keep_p + 8, LANE), F32),
            pltpu.VMEM((sums, col_n, 8, LANE), F32),
            pltpu.VMEM((sums, row_n, 8, LANE), F32),
            pltpu.VMEM((STEPS, row_n, v_sub, tile), BF16),
            pltpu.VMEM((STEPS, col_n, u_sub, tile), BF16),
            pltpu.VMEM((col_n, u_sub, tile), F32),
            pltpu.VMEM((row_n, v_sub, tile), F32),
            pltpu.VMEM((STEPS, col_n, u_sub, tile), F32),
            pltpu.VMEM((STEPS, row_n, v_sub, tile), F32),
            pltpu.VMEM((slots, tile), F32),
            pltpu.VMEM((slots, tile), F32),
            dma((3,)),
            dma((col_n,)),
            dma((col_n,)),
            dma((row_n,)),
            dma((row_n,)),
            dma((max(row_n, col_n),)),
            dma((sums + 1, col_n)),
            dma((sums + 1, row_n)),
            dma((STEPS, row_n)),
            dma((STEPS, col_n)),
            dma((STEPS, col_n)),
            dma((STEPS, row_n)),
        ],
        compiler_params=pltpu.CompilerParams(
            collective_id=0, has_side_effects=True, vmem_limit_bytes=48 * 1024 * 1024
        ),
    )(
        u_start, v_start, jnp.pad(keep_u.T, pad), jnp.pad(keep_v.T, pad), v_next.reshape(1, -1), tile_blocks,
        tile_rows.reshape(1, -1), tile_cols.reshape(1, -1), tile_count.reshape(1, 1),
    )
    return u_basis, v_basis, bidiagonal[:2, :STEPS]


def solution(mesh):
    return jax.shard_map(
        per_device,
        mesh=mesh,
        in_specs=(
            P("col", "row"),
            P("row", "col"),
            P(),
            P(),
            P(("col", "row")),
            P(("row", "col"), None, None),
            P(("row", "col")),
            P(("row", "col")),
            P(("row", "col")),
        ),
        out_specs=(P(None, ("row", "col")), P(None, ("col", "row")), P()),
        check_vma=False,
    )
```

```python
import functools

import jax
import jax.numpy as jnp
from jax import lax
from jax.experimental import pallas as pl
from jax.experimental.pallas import tpu as pltpu
from jax.sharding import PartitionSpec as P

STEPS = 2
HIGH = lax.Precision.HIGHEST
F32 = jnp.float32
BF16 = jnp.bfloat16
LANE = 128
HALF = 64
DIRECT = 32


def kernel(
    row_n, col_n, keep_n, u_hbm, v_hbm, keep_u, keep_v, v_next, tiles_hbm, rows_ref, cols_ref, count_ref,
    u_out, v_out, bi_out,
    u_all, v_all, tiles, u_rows, v_rows, u_vec, v_vec, big_col, big_row, sum_col, sum_row, sum_all,
    v_gather, u_gather, u_parts, v_parts, u_recv, v_recv, picked, products,
    local_sem, init_u_send, init_u_recv, init_v_send, init_v_recv, send_sem,
    sum_col_sem, sum_row_sem, sum_all_sem, big_col_send, big_col_sem, big_row_send, big_row_sem,
    vg_sem, ug_sem, ur_sem, vr_sem,
):
    row_me = lax.axis_index("row")
    col_me = lax.axis_index("col")
    barrier = pltpu.get_barrier_semaphore()
    direct = row_n * col_n <= DIRECT
    peers = [(a, b) for a in range(row_n) for b in range(col_n)
             if (a or b) and (direct or not (a and b))]
    for a, b in peers:
        where = {"row": lax.rem(row_me + a, row_n), "col": lax.rem(col_me + b, col_n)}
        pl.semaphore_signal(barrier, inc=1, device_id=where, device_id_type=pl.DeviceIdType.MESH)

    u_here, v_here = u_hbm.shape[0], v_hbm.shape[0]
    u_len, v_len = u_rows.shape[1], v_rows.shape[1]
    u_total = float(u_len * row_n * col_n)
    v_total = float(v_len * row_n * col_n)
    rows_p = u_rows.shape[0]
    keep_p = keep_u.shape[0]
    tile = tiles.shape[1]
    slots = tiles.shape[0]
    u_sub, v_sub = u_len // tile, v_len // tile

    def u_src(p):
        return u_hbm.at[:, pl.ds(pl.multiple_of(p * u_len, LANE), u_len)]

    def v_src(p):
        return v_hbm.at[:, pl.ds(pl.multiple_of(p * v_len, LANE), v_len)]

    u_dst = u_all.at[pl.ds(pl.multiple_of(col_me * u_here, 8), u_here), :]
    v_dst = v_all.at[pl.ds(pl.multiple_of(row_me * v_here, 8), v_here), :]
    own_v = pltpu.make_async_copy(v_src(row_me), v_dst, local_sem.at[0])
    own_u = pltpu.make_async_copy(u_src(col_me), u_dst, local_sem.at[1])
    own_t = pltpu.make_async_copy(tiles_hbm, tiles, local_sem.at[2])
    own_v.start()
    own_u.start()
    own_t.start()

    def send(axis, me, n, src, dst, sends, recvs):
        copies = []
        for k in range(1, n):
            target = lax.rem(me + k, n)
            copy = pltpu.make_async_remote_copy(
                src_ref=src(target, k), dst_ref=dst(k), send_sem=sends.at[k], recv_sem=recvs(k),
                device_id={axis: target}, device_id_type=pl.DeviceIdType.MESH)
            copy.start()
            copies.append(copy)
        return copies

    pl.semaphore_wait(barrier, len(peers))
    v_init = send("row", row_me, row_n, lambda p, k: v_src(p), lambda k: v_dst, init_v_send,
                  lambda k: init_v_recv.at[k])
    u_init = send("col", col_me, col_n, lambda p, k: u_src(p), lambda k: u_dst, init_u_send,
                  lambda k: init_u_recv.at[k])

    active = lax.broadcasted_iota(jnp.int32, (1, slots), 1) < count_ref[...]
    row_blocks = u_parts.shape[0] * u_sub
    col_blocks = v_parts.shape[0] * v_sub
    row_hot = jnp.where(
        (lax.broadcasted_iota(jnp.int32, (row_blocks, slots), 0) == rows_ref[...]) & active, 1.0, 0.0)
    col_hot = jnp.where(
        (lax.broadcasted_iota(jnp.int32, (col_blocks, slots), 0) == cols_ref[...]) & active, 1.0, 0.0)

    eye = (lax.broadcasted_iota(jnp.int32, (rows_p, LANE), 0)
           == lax.broadcasted_iota(jnp.int32, (rows_p, LANE), 1))
    row_id = lax.broadcasted_iota(jnp.int32, (rows_p, LANE), 0)
    lane_id = lax.broadcasted_iota(jnp.int32, (rows_p, LANE), 1)
    lane_row = lax.broadcasted_iota(jnp.int32, (1, LANE), 1)

    def to_row(column):
        return jnp.sum(jnp.where(eye, column, 0.0), axis=0, keepdims=True)

    def to_column(row):
        return jnp.sum(jnp.where(eye, row, 0.0), axis=1, keepdims=True)

    def add_up(buf, n):
        parts = [buf[i] for i in range(n)]
        while len(parts) > 1:
            parts = [parts[i] + parts[i + 1] if i + 1 < len(parts) else parts[i]
                     for i in range(0, len(parts), 2)]
        return parts[0]

    def col_start(buf, value, sends, recvs):
        buf[col_me] = value
        return send("col", col_me, col_n, lambda p, k: buf.at[col_me], lambda k: buf.at[col_me],
                    sends, recvs)

    def row_start(buf, value, sends, recvs):
        buf[row_me] = value
        return send("row", row_me, row_n, lambda p, k: buf.at[row_me], lambda k: buf.at[row_me],
                    sends, recvs)

    def sum_start(row, index):
        if not direct:
            return col_start(sum_col.at[index], row, send_sem, lambda k: sum_col_sem.at[index, k])
        me = row_me * col_n + col_me
        buf = sum_all.at[index]
        buf[me] = row
        copies = []
        for k, (a, b) in enumerate(peers):
            where = {"row": lax.rem(row_me + a, row_n), "col": lax.rem(col_me + b, col_n)}
            copy = pltpu.make_async_remote_copy(
                src_ref=buf.at[me], dst_ref=buf.at[me], send_sem=send_sem.at[k],
                recv_sem=sum_all_sem.at[index, k], device_id=where,
                device_id_type=pl.DeviceIdType.MESH)
            copy.start()
            copies.append(copy)
        return copies

    def sum_finish(copies, index):
        for copy in copies:
            copy.wait()
        if direct:
            return add_up(sum_all.at[index], row_n * col_n)
        buf = sum_row.at[index]
        for copy in row_start(buf, add_up(sum_col.at[index], col_n), send_sem,
                              lambda k: sum_row_sem.at[index, k]):
            copy.wait()
        return add_up(buf, row_n)

    def coef(basis, vec):
        acc = jnp.zeros((rows_p, LANE), F32)
        for j in range(vec.shape[1] // LANE):
            at = slice(j * LANE, (j + 1) * LANE)
            acc = acc + basis[:, at] * vec[:, at]
        return to_row(jnp.sum(acc, axis=1, keepdims=True))

    def remove(basis, vec, column):
        spread = jnp.broadcast_to(column, (rows_p, LANE))
        square = jnp.zeros((1, LANE), F32)
        for j in range(vec.shape[1] // LANE):
            at = slice(j * LANE, (j + 1) * LANE)
            new = vec[:, at] - jnp.sum(spread * basis[:, at], axis=0, keepdims=True)
            vec[:, at] = new
            square = square + new * new
        return jnp.sum(square, axis=1, keepdims=True)

    def orth(basis, vec, first_sum, index, length, gram_now, place, between=lambda: None):
        first = first_sum / length
        square = remove(basis, vec, to_column(first))
        copies = sum_start(coef(basis, vec) + jnp.where(lane_row == LANE - 1, square, 0.0), index)
        between()
        got = sum_finish(copies, index)
        square = jnp.sum(jnp.where(lane_row == LANE - 1, got, 0.0), axis=1, keepdims=True) / length
        second = jnp.where(lane_row < rows_p, got, 0.0) / length
        second_col = to_column(second)
        remove(basis, vec, second_col)
        gram = gram_now()
        gram_coef = jnp.sum(gram * second_col, axis=0, keepdims=True)
        square = (square - 2.0 * jnp.sum(second * second, axis=1, keepdims=True)
                  + jnp.sum(second * gram_coef, axis=1, keepdims=True))
        scale = jnp.sqrt(square + 1e-06)
        inverse = 1.0 / scale
        vec[...] = vec[...] * inverse

        def grow():
            basis[place:place + 1, :] = vec[...]
            cross = (second - gram_coef) * inverse
            grown = jnp.where(row_id == place, cross, gram)
            grown = jnp.where(lane_id == place, to_column(cross), grown)
            corner = (row_id == place) & (lane_id == place)
            return jnp.where(corner, square / (scale * scale), grown)

        return scale, grow

    def matvec(gathered, n, pick_hot, put_hot, contract):
        full = jnp.concatenate([gathered[i].astype(F32) for i in range(n)], axis=0).astype(BF16)
        picked[...] = lax.dot_general(pick_hot.astype(BF16), full, (((0,), (0,)), ((), ())),
                                      preferred_element_type=F32)
        sub = lax.broadcasted_iota(jnp.int32, (8, tile), 0)

        def group(g, carry):
            base = pl.multiple_of(g * 8, 8)
            left = picked[pl.ds(base, 8), :].astype(BF16)
            acc = jnp.zeros((8, tile), F32)
            for i in range(8):
                res = lax.dot_general(left, tiles[base + i], (((1,), (contract,)), ((), ())),
                                      preferred_element_type=F32)
                acc = jnp.where(sub == i, res, acc)
            products[pl.ds(base, 8), :] = acc
            return carry

        lax.fori_loop(0, slots // 8, group, 0)
        return jnp.dot(put_hot, products[...], precision=HIGH, preferred_element_type=F32)

    def gather(axis, me, n, vec, sub, buf, sems, grow):
        own = jnp.concatenate([vec[:, i * tile:(i + 1) * tile] for i in range(sub)], axis=0)
        buf[me] = own.astype(BF16)
        copies = send(axis, me, n, lambda p, k: buf.at[me], lambda k: buf.at[me], send_sem, sems)
        gram = grow()
        for copy in copies:
            copy.wait()
        return gram

    def scatter(axis, me, n, value, vec, sub, parts, recv, sems):
        for i in range(n):
            parts[i] = value[i * sub:(i + 1) * sub, :]
        for copy in send(axis, me, n, lambda p, k: parts.at[p], lambda k: recv.at[k], send_sem, sems):
            copy.wait()
        total = parts[me]
        for k in range(1, n):
            total = total + recv[k]
        for i in range(sub):
            vec[:, i * tile:(i + 1) * tile] = total[i:i + 1, :]

    u_rows[...] = jnp.zeros(u_rows.shape, F32)
    v_rows[...] = jnp.zeros(v_rows.shape, F32)
    v_vec[...] = v_next[...]
    own_v.wait()
    for copy in v_init:
        copy.wait()

    def kept(keep, source, target, length):
        for j in range(length // 512):
            at = slice(j * 512, (j + 1) * 512)
            target[0:keep_p, at] = jnp.dot(keep[...], source[:, at], precision=HIGH,
                                           preferred_element_type=F32)

    def half_gram(basis):
        small = basis[0:keep_p, :]
        wide = jnp.concatenate([basis[...], jnp.zeros((HALF - rows_p, basis.shape[1]), F32)], axis=0)
        return lax.dot_general(small, wide, (((1,), (1,)), ((), ())), precision=HIGH,
                               preferred_element_type=F32)

    kept(keep_v, v_all, v_rows, v_len)
    first_copies = sum_start(coef(v_rows, v_vec), 0)
    own_u.wait()
    for copy in u_init:
        copy.wait()
    kept(keep_u, u_all, u_rows, u_len)
    both = jnp.concatenate([half_gram(v_rows), half_gram(u_rows)], axis=1)
    gram_copies = col_start(big_col, both, big_col_send, lambda k: big_col_sem.at[k])

    def gram_step():
        for copy in gram_copies:
            copy.wait()
        gram_copies[:] = row_start(big_row, add_up(big_col, col_n), big_row_send,
                                   lambda k: big_row_sem.at[k])

    def gram_end():
        for copy in gram_copies:
            copy.wait()
        total = add_up(big_row, row_n)
        total = jnp.concatenate([total, jnp.zeros((rows_p - keep_p, LANE), F32)], axis=0)
        grams.append(jnp.where(lane_id < HALF, pltpu.roll(total, HALF, 1), 0.0) / u_total)
        return jnp.where(lane_id < HALF, total, 0.0) / v_total

    grams = []
    scale, grow = orth(v_rows, v_vec, sum_finish(first_copies, 0), 1, v_total, gram_end, keep_n,
                       gram_step)
    gram_u = grams[0]
    index = 2
    alphas, betas = [], []
    for step in range(STEPS):
        gram_v = gather("row", row_me, row_n, v_vec, v_sub, v_gather.at[step],
                        lambda k: vg_sem.at[step, k], grow)
        if step == 0:
            own_t.wait()
        partial = matvec(v_gather.at[step], row_n, col_hot, row_hot, 1)
        scatter("col", col_me, col_n, partial, u_vec, u_sub, u_parts, u_recv.at[step],
                lambda k: ur_sem.at[step, k])
        total = sum_finish(sum_start(coef(u_rows, u_vec), index), index)
        alpha, grow = orth(u_rows, u_vec, total, index + 1, u_total, lambda: gram_u, keep_n + step)
        gram_u = gather("col", col_me, col_n, u_vec, u_sub, u_gather.at[step],
                        lambda k: ug_sem.at[step, k], grow)
        partial = matvec(u_gather.at[step], col_n, row_hot, col_hot, 0)
        scatter("row", row_me, row_n, partial, v_vec, v_sub, v_parts, v_recv.at[step],
                lambda k: vr_sem.at[step, k])
        total = sum_finish(sum_start(coef(v_rows, v_vec), index + 2), index + 2)
        beta, grow = orth(v_rows, v_vec, total, index + 3, v_total, lambda: gram_v, keep_n + 1 + step)
        index += 4
        alphas.append(alpha)
        betas.append(beta)
    grow()
    place_r = lax.broadcasted_iota(jnp.int32, (8, LANE), 0)
    place_l = lax.broadcasted_iota(jnp.int32, (8, LANE), 1)
    result = jnp.zeros((8, LANE), F32)
    for step in range(STEPS):
        result = jnp.where((place_r == 0) & (place_l == step), alphas[step], result)
        result = jnp.where((place_r == 1) & (place_l == step), betas[step], result)
    bi_out[...] = result
    u_out[...] = u_rows[0:u_out.shape[0], :]
    v_out[...] = v_rows[0:v_out.shape[0], :]


def per_device(
    u_start, v_start, keep_u, keep_v, v_next, tile_blocks, tile_rows, tile_cols, tile_count
):
    row_n = lax.axis_size("row")
    col_n = lax.axis_size("col")
    u_here, v_here = u_start.shape[0], v_start.shape[0]
    basis, keep_n = keep_u.shape
    u_len = u_start.shape[1] // col_n
    v_len = v_start.shape[1] // row_n
    slots, tile = tile_blocks.shape[0], tile_blocks.shape[1]
    rows_p = -(-(keep_n + 1 + STEPS) // 8) * 8
    keep_p = -(-keep_n // 8) * 8
    assert rows_p <= HALF
    pad = ((0, keep_p - keep_n), (0, 0))
    sums = 2 + 4 * STEPS
    total_n = row_n * col_n
    direct_n = total_n if total_n <= DIRECT else 1
    staged = 1 if total_n <= DIRECT else sums
    dma = pltpu.SemaphoreType.DMA
    vmem = pl.BlockSpec(memory_space=pltpu.VMEM)
    hbm = pl.BlockSpec(memory_space=pl.ANY)
    u_sub, v_sub = u_len // tile, v_len // tile
    u_basis, v_basis, bidiagonal = pl.pallas_call(
        functools.partial(kernel, row_n, col_n, keep_n),
        out_shape=(
            jax.ShapeDtypeStruct((keep_n + STEPS, u_len), F32),
            jax.ShapeDtypeStruct((keep_n + 1 + STEPS, v_len), F32),
            jax.ShapeDtypeStruct((8, LANE), F32),
        ),
        in_specs=[hbm, hbm, vmem, vmem, vmem, hbm, vmem, vmem, vmem],
        out_specs=(vmem, vmem, vmem),
        scratch_shapes=[
            pltpu.VMEM((basis, u_len), F32),
            pltpu.VMEM((basis, v_len), F32),
            pltpu.VMEM(tile_blocks.shape, BF16),
            pltpu.VMEM((rows_p, u_len), F32),
            pltpu.VMEM((rows_p, v_len), F32),
            pltpu.VMEM((1, u_len), F32),
            pltpu.VMEM((1, v_len), F32),
            pltpu.VMEM((col_n, keep_p, LANE), F32),
            pltpu.VMEM((row_n, keep_p, LANE), F32),
            pltpu.VMEM((staged, col_n, 1, LANE), F32),
            pltpu.VMEM((staged, row_n, 1, LANE), F32),
            pltpu.VMEM((sums, direct_n, 1, LANE), F32),
            pltpu.VMEM((STEPS, row_n, v_sub, tile), BF16),
            pltpu.VMEM((STEPS, col_n, u_sub, tile), BF16),
            pltpu.VMEM((col_n, u_sub, tile), F32),
            pltpu.VMEM((row_n, v_sub, tile), F32),
            pltpu.VMEM((STEPS, col_n, u_sub, tile), F32),
            pltpu.VMEM((STEPS, row_n, v_sub, tile), F32),
            pltpu.VMEM((slots, tile), F32),
            pltpu.VMEM((slots, tile), F32),
            dma((3,)),
            dma((col_n,)),
            dma((col_n,)),
            dma((row_n,)),
            dma((row_n,)),
            dma((max(row_n, col_n, direct_n),)),
            dma((staged, col_n)),
            dma((staged, row_n)),
            dma((sums, direct_n)),
            dma((col_n,)),
            dma((col_n,)),
            dma((row_n,)),
            dma((row_n,)),
            dma((STEPS, row_n)),
            dma((STEPS, col_n)),
            dma((STEPS, col_n)),
            dma((STEPS, row_n)),
        ],
        compiler_params=pltpu.CompilerParams(
            collective_id=0, has_side_effects=True, vmem_limit_bytes=48 * 1024 * 1024
        ),
    )(
        u_start, v_start, jnp.pad(keep_u.T, pad), jnp.pad(keep_v.T, pad), v_next.reshape(1, -1), tile_blocks,
        tile_rows.reshape(1, -1), tile_cols.reshape(1, -1), tile_count.reshape(1, 1),
    )
    return u_basis, v_basis, bidiagonal[:2, :STEPS]


def solution(mesh):
    return jax.shard_map(
        per_device,
        mesh=mesh,
        in_specs=(
            P("col", "row"),
            P("row", "col"),
            P(),
            P(),
            P(("col", "row")),
            P(("row", "col"), None, None),
            P(("row", "col")),
            P(("row", "col")),
            P(("row", "col")),
        ),
        out_specs=(P(None, ("row", "col")), P(None, ("col", "row")), P()),
        check_vma=False,
    )
```
